512 devices in a mesh: blk: 32 (over x, y, core), rhs: 16 (over z).
Axes of the slice: x: 4, y: 4, z: 16, core: 2. Of those that a mesh axis runs over, the one named last changes fastest.
Arguments:
- lower_coupling: bfloat16 [2, 2048, 4096], P(None, 'blk'), may hold values from -0.0625 to 0.0625
- upper_coupling: bfloat16 [2, 2048, 4096], P(None, 'blk'), may hold values from -0.0625 to 0.0625
- lower_inverse: bfloat16 [2, 2048, 2048], P(None, 'blk'), may hold values from -1 to 2
- upper_inverse: bfloat16 [2, 2048, 2048], P(None, 'blk'), may hold values from -1 to 2
- right_side: float32 [2, 2048, 16384], P(None, 'blk', 'rhs'), parts along dimension 2, may hold values from -6 to 6
Outputs:
- solution: float32 [2, 2048, 16384], P(None, 'blk', 'rhs'), parts along dimension 2
The draws below stay inside these ranges and needn't reach their ends.
There are 16 independent parts, one for each index of `rhs`. The reference program is written for one: setup_inputs(seed, part) draws one part's arguments, and reference() takes and returns one part's arrays. A program takes and returns all parts, laid end to end along the dimension named above; an argument that names none is the same for every part. Nothing has to cross between parts.
All inputs are finite; a program needn't handle non-finite values.
Results may differ from the reference program's by a relative error of at most 0.0043.
Values may be sent and summed in bfloat16 or wider, within the bound.
A program may use at most 64 MiB of HBM per device.

```python
import jax
import jax.numpy as jnp

SEP = 2048
NSUP = 2
RHS = 1024
ORDER = 4096


def inverse_blocks(key):
    noise = jnp.clip(jax.random.normal(key, (NSUP, SEP, SEP), jnp.float32), -6.0, 6.0)
    eye_block = jnp.eye(SEP, dtype=jnp.float32)[None, :, :]
    return (eye_block + 0.7 * noise / jnp.sqrt(jnp.float32(SEP))).astype(jnp.bfloat16)


def draw_lower_inverse(key, part):
    return inverse_blocks(jax.random.fold_in(key, 11))


def draw_upper_inverse(key, part):
    return inverse_blocks(jax.random.fold_in(key, 23))


def levels(stream_key, dims, cuts, smallest, high):
    def one(dim, parts):
        draws = jax.random.uniform(jax.random.fold_in(jax.random.fold_in(stream_key, 6), dim), (parts,), jnp.float32, smallest / len(cuts), high / len(cuts))
        return jnp.repeat(jnp.exp(draws), dims[dim] // parts).reshape((-1,) + (1,) * (len(dims) - dim - 1))

    level = one(*cuts[0])
    for cut in cuts[1:]:
        level = level * one(*cut)
    return level


def gaussian(rng, dims, deviation, limit, shards=(), kind=jnp.bfloat16):
    values = jax.random.normal(rng, dims, jnp.float32) * deviation
    if len(shards) > 0:
        values = levels(rng, dims, shards, -0.22, 0.18) * values
    return jnp.clip(values, min=-limit, max=limit).astype(kind)


def setup_inputs(seed: int = 0, part: int = 0) -> dict:
    key_list = jax.random.split(jax.random.key(seed), 6)
    part_keys = jax.random.split(jax.random.fold_in(key_list[5], part), 6)
    lower_coupling = gaussian(key_list[0], (NSUP, SEP, ORDER), (2 * ORDER) ** -0.5, 0.0625, ((1, 32),))
    upper_coupling = gaussian(key_list[1], (NSUP, SEP, ORDER), (2 * ORDER) ** -0.5, 0.0625, ((1, 32),))
    lower_inverse = draw_lower_inverse(jax.random.fold_in(key_list[5], 71), part)
    upper_inverse = draw_upper_inverse(jax.random.fold_in(key_list[5], 71), part)
    right_side = gaussian(part_keys[4], (NSUP, SEP, RHS), 1.0, 6.0, ((1, 32),), jnp.float32)
    return dict(lower_coupling=lower_coupling, upper_coupling=upper_coupling, lower_inverse=lower_inverse, upper_inverse=upper_inverse, right_side=right_side)


def reference(lower_coupling, upper_coupling, lower_inverse, upper_inverse, right_side):
    forward_halves = []
    forward_solved = []
    for step in range(NSUP):
        residual = right_side[step]
        for other in range(step):
            columns = lower_coupling[step][:, other * SEP:(other + 1) * SEP]
            residual = residual - jnp.dot(columns, forward_halves[other], preferred_element_type=jnp.float32)
        rounded = residual.astype(jnp.bfloat16)
        forward_halves.append(rounded)
        forward_solved.append(jnp.dot(lower_inverse[step], rounded, preferred_element_type=jnp.float32))
    backward_halves = [None] * NSUP
    results = [None] * NSUP
    for step in range(NSUP - 1, -1, -1):
        residual = forward_solved[step]
        for other in range(step + 1, NSUP):
            columns = upper_coupling[step][:, other * SEP:(other + 1) * SEP]
            residual = residual - jnp.dot(columns, backward_halves[other], preferred_element_type=jnp.float32)
        rounded = residual.astype(jnp.bfloat16)
        backward_halves[step] = rounded
        results[step] = jnp.dot(upper_inverse[step], rounded, preferred_element_type=jnp.float32)
    return jnp.stack(results)
```

```python
import functools

import jax
import jax.numpy as jnp
from jax import lax
from jax.experimental import pallas as pl
from jax.experimental.pallas import tpu as pltpu
from jax.sharding import Mesh
from jax.sharding import PartitionSpec as P

BLK = ("blk_0", "blk_1", "blk_2")
L10, LI1, U01, LI0, UI1, UI0 = range(6)


def kernel(
    depth_z, lc, li, uc, ui, b, o,
    w, v, bv, fst, b1g, acc, y0, ob, ro,
    hsem, ysend, yrecv, msend, mrecv, asend, arecv, bsend, brecv, xsend, xrecv,
):
    rows, cols = fst.shape[1], fst.shape[2]
    own = 4 * rows
    span = 2 * rows
    x, y, k, z = (lax.axis_index(a) for a in BLK + ("rhs",))
    xr, xl, xo = (x + 1) % 4, (x + 3) % 4, (x + 2) % 4
    yr, yl, yo = (y + 1) % 4, (y + 3) % 4, (y + 2) % 4
    zr, zl = (z + 1) % depth_z, (z + depth_z - 1) % depth_z
    p = z % 2
    q = 1 - p
    sib = 1 - k
    RIGHT, LEFT = (xr, y, k, z), (xl, y, k, z)
    UP, DOWN = (x, yr, k, z), (x, yl, k, z)
    NEXT, BACK = (x, y, k, zr), (x, y, k, zl)
    SIB = (x, y, sib, z)

    def remote(src, dst, ssem, rsem, dev):
        return pltpu.make_async_remote_copy(
            src_ref=src, dst_ref=dst, send_sem=ssem, recv_sem=rsem,
            device_id=dev, device_id_type=pl.DeviceIdType.MESH,
        )

    sent = []

    def send(src, sends, recvs, i, dev, dst=None):
        c = remote(src, src if dst is None else dst, sends.at[i], recvs.at[i], dev)
        c.start()
        sent.append(c)

    def arrived(ref, sends, recvs, i, dev):
        remote(ref, ref, sends.at[i], recvs.at[i], dev).wait_recv()

    barrier = pltpu.get_barrier_semaphore()
    greeted = [RIGHT, LEFT, (xo, y, k, z), UP, DOWN, SIB, NEXT, BACK]
    for dev in greeted:
        pl.semaphore_signal(barrier, inc=1, device_id=dev, device_id_type=pl.DeviceIdType.MESH)

    loads_b = [
        [
            pltpu.make_async_copy(b.at[s, :, c * cols:(c + 1) * cols], bv.at[s, c], hsem.at[s, c])
            for c in range(4)
        ]
        for s in range(2)
    ]
    sep = 32 * rows
    source = [
        lc.at[1, :, :, :, 0:sep], li.at[1], uc.at[0, :, :, :, sep:2 * sep],
        li.at[0], ui.at[1], ui.at[0],
    ]
    loads_w = [pltpu.make_async_copy(source[m], w.at[m, x], hsem.at[2 + m // 4, m % 4]) for m in range(6)]
    for c in loads_b[0]:
        c.start()
    loads_w[0].start()
    for c in loads_b[1]:
        c.start()
    for c in loads_w[1:]:
        c.start()
    for c in range(4):
        loads_b[0][c].wait()
        fst[c] = bv[0, c].astype(jnp.bfloat16)
    v[0, x, y, k] = fst[x]

    pl.semaphore_wait(barrier, len(greeted))

    def own_send(m):
        loads_w[m].wait()
        send(w.at[m, x, p], msend.at[m], mrecv.at[m], 0, RIGHT)
        send(w.at[m, x, p], msend.at[m], mrecv.at[m], 1, LEFT)

    def relay(m):
        s, r = msend.at[m], mrecv.at[m]
        arrived(w.at[m, xl, p], s, r, 0, LEFT)
        send(w.at[m, xl, p, 0], s, r, 2, RIGHT)
        send(w.at[m, xl, p, 0], s, r, 4, NEXT)
        send(w.at[m, xl, p, 1], s, r, 5, BACK)
        arrived(w.at[m, xr, p], s, r, 1, RIGHT)
        send(w.at[m, xr, p, 1], s, r, 3, LEFT)
        send(w.at[m, xr, p, 0], s, r, 6, NEXT)
        send(w.at[m, xr, p, 1], s, r, 7, BACK)

    def relay_far(m):
        s, r = msend.at[m], mrecv.at[m]
        arrived(w.at[m, xo, p, 0], s, r, 2, LEFT)
        send(w.at[m, xo, p, 0], s, r, 8, NEXT)
        arrived(w.at[m, xo, p, 1], s, r, 3, RIGHT)
        send(w.at[m, xo, p, 1], s, r, 9, BACK)

    def complete(m):
        s, r = msend.at[m], mrecv.at[m]
        for i, (src, part) in enumerate([(xl, 0), (xl, 1), (xr, 0), (xr, 1), (xo, 0), (xo, 1)]):
            arrived(w.at[m, src, q, part], s, r, 4 + i, BACK if part == 0 else NEXT)

    def product(m, s, yy):
        lhs = jnp.concatenate(
            [
                w[m, :, :, :, :, pl.ds(pl.multiple_of(c * 4 * span + yy * span, span), span)].reshape(own, span)
                for c in range(4)
            ],
            axis=1,
        )
        rhs = v[s, :, yy].reshape(4 * span, cols)
        return jnp.dot(lhs, rhs, preferred_element_type=jnp.float32)

    def full_product(m, s, dst):
        dst[...] = product(m, s, 0)
        for yy in range(1, 4):
            dst[...] += product(m, s, yy)

    def gather(s, m, early=None, middle=None, late=None):
        ss, rr = ysend.at[s], yrecv.at[s]
        mine = v.at[s, :, y, k]
        send(v.at[s, 0:2, y, k], ss, rr, 0, UP)
        send(v.at[s, 2:4, y, k], ss, rr, 2, DOWN)
        send(v.at[s, 2:4, y, k], ss, rr, 1, UP)
        send(v.at[s, 0:2, y, k], ss, rr, 3, DOWN)
        send(mine, ss, rr, 6, SIB)
        if early is not None:
            early()
        arrived(v.at[s, 0:2, yl, k], ss, rr, 0, DOWN)
        send(v.at[s, 0:2, yl, k], ss, rr, 4, UP)
        send(v.at[s, 0:2, yl, k], ss, rr, 7, SIB)
        arrived(v.at[s, 2:4, yr, k], ss, rr, 2, UP)
        send(v.at[s, 2:4, yr, k], ss, rr, 5, DOWN)
        send(v.at[s, 2:4, yr, k], ss, rr, 9, SIB)
        if middle is not None:
            middle()
        arrived(v.at[s, :, y, sib], ss, rr, 6, SIB)
        acc[...] = product(m, s, y)
        arrived(v.at[s, 2:4, yl, k], ss, rr, 1, DOWN)
        send(v.at[s, 2:4, yl, k], ss, rr, 8, SIB)
        arrived(v.at[s, 0:2, yr, k], ss, rr, 3, UP)
        send(v.at[s, 0:2, yr, k], ss, rr, 10, SIB)
        if late is not None:
            late()
        arrived(v.at[s, 0:2, yl, sib], ss, rr, 7, SIB)
        arrived(v.at[s, 2:4, yl, sib], ss, rr, 8, SIB)
        acc[...] += product(m, s, yl)
        arrived(v.at[s, 0:2, yo, k], ss, rr, 4, DOWN)
        send(v.at[s, 0:2, yo, k], ss, rr, 11, SIB)
        arrived(v.at[s, 2:4, yo, k], ss, rr, 5, UP)
        send(v.at[s, 2:4, yo, k], ss, rr, 12, SIB)
        arrived(v.at[s, 2:4, yr, sib], ss, rr, 9, SIB)
        arrived(v.at[s, 0:2, yr, sib], ss, rr, 10, SIB)
        acc[...] += product(m, s, yr)
        arrived(v.at[s, 0:2, yo, sib], ss, rr, 11, SIB)
        arrived(v.at[s, 2:4, yo, sib], ss, rr, 12, SIB)
        acc[...] += product(m, s, yo)

    def result(s):
        ob[s] = acc[...].reshape(4, rows, cols).astype(jnp.bfloat16)
        for d in (2, 1, 3):
            send(ob.at[s, (x + d) % 4], xsend.at[s], xrecv.at[s], d, ((x + d) % 4, y, k, z), ro.at[s, x])

    def write(s):
        ro[s, x] = ob[s, x]
        for d in (1, 3, 2):
            arrived(ro.at[s, (x + 4 - d) % 4], xsend.at[s], xrecv.at[s], d, ((x + 4 - d) % 4, y, k, z))
        for c in range(4):
            o[s, :, c * cols:(c + 1) * cols] = ro[s, c].astype(jnp.float32)

    for d in (2, 1, 3):
        send(fst.at[(x + d) % 4], asend, arecv, d, ((x + d) % 4, y, k, z), v.at[0, x, y, k])
    own_send(L10)
    for d in (1, 3, 2):
        arrived(v.at[0, (x + 4 - d) % 4, y, k], asend, arecv, d, ((x + 4 - d) % 4, y, k, z))

    def middle_0():
        relay(L10)
        own_send(LI1)
        for c in loads_b[1]:
            c.wait()
        b1g[x] = bv[1, x]
        for d in (2, 1, 3):
            send(bv.at[1, (x + d) % 4], bsend, brecv, d, ((x + d) % 4, y, k, z), b1g.at[x])

    def late_0():
        relay_far(L10)
        relay(LI1)
        own_send(U01)
        complete(L10)

    def gather_first():
        s = 0
        ss, rr = ysend.at[s], yrecv.at[s]
        send(v.at[s, 0:2, y, k], ss, rr, 0, UP)
        send(v.at[s, 2:4, y, k], ss, rr, 2, DOWN)
        send(v.at[s, 2:4, y, k], ss, rr, 1, UP)
        send(v.at[s, 0:2, y, k], ss, rr, 3, DOWN)
        send(v.at[s, :, y, k], ss, rr, 6, SIB)
        arrived(v.at[s, 0:2, yl, k], ss, rr, 0, DOWN)
        send(v.at[s, 0:2, yl, k], ss, rr, 4, UP)
        send(v.at[s, 0:2, yl, k], ss, rr, 7, SIB)
        arrived(v.at[s, 2:4, yr, k], ss, rr, 2, UP)
        send(v.at[s, 2:4, yr, k], ss, rr, 5, DOWN)
        send(v.at[s, 2:4, yr, k], ss, rr, 9, SIB)
        middle_0()
        arrived(v.at[s, 2:4, yl, k], ss, rr, 1, DOWN)
        send(v.at[s, 2:4, yl, k], ss, rr, 8, SIB)
        arrived(v.at[s, 0:2, yr, k], ss, rr, 3, UP)
        send(v.at[s, 0:2, yr, k], ss, rr, 10, SIB)
        arrived(v.at[s, 0:2, yo, k], ss, rr, 4, DOWN)
        send(v.at[s, 0:2, yo, k], ss, rr, 11, SIB)
        arrived(v.at[s, 2:4, yo, k], ss, rr, 5, UP)
        send(v.at[s, 2:4, yo, k], ss, rr, 12, SIB)
        late_0()
        arrived(v.at[s, :, y, sib], ss, rr, 6, SIB)
        arrived(v.at[s, 0:2, yl, sib], ss, rr, 7, SIB)
        arrived(v.at[s, 2:4, yl, sib], ss, rr, 8, SIB)
        arrived(v.at[s, 2:4, yr, sib], ss, rr, 9, SIB)
        arrived(v.at[s, 0:2, yr, sib], ss, rr, 10, SIB)
        arrived(v.at[s, 0:2, yo, sib], ss, rr, 11, SIB)
        arrived(v.at[s, 2:4, yo, sib], ss, rr, 12, SIB)
        full_product(L10, 0, acc)

    gather_first()
    for d in (1, 3, 2):
        arrived(b1g.at[(x + 4 - d) % 4], bsend, brecv, d, ((x + 4 - d) % 4, y, k, z))

    def residual(s, values):
        v[s, :, y, k] = values.astype(jnp.bfloat16).reshape(4, rows, cols)

    residual(1, b1g[...].reshape(own, cols) - acc[...])

    def middle_1():
        relay_far(LI1)
        relay(U01)
        own_send(LI0)
        complete(LI1)

    gather(1, LI1, middle=middle_1, late=lambda: relay_far(U01))

    residual(2, acc[...])

    def early_2():
        relay(LI0)
        own_send(UI1)
        complete(U01)

    def middle_2():
        relay_far(LI0)
        relay(UI1)
        own_send(UI0)

    def late_2():
        complete(LI0)
        full_product(LI0, 0, y0)
        relay_far(UI1)

    gather(2, U01, early=early_2, middle=middle_2, late=late_2)

    residual(3, y0[...] - acc[...])

    def early_3():
        relay(UI0)

    def middle_3():
        complete(UI1)
        full_product(UI1, 2, acc)
        result(1)
        relay_far(UI0)
        complete(UI0)

    gather(3, UI0, early=early_3, middle=middle_3)
    result(0)
    write(1)
    write(0)
    for c in sent:
        c.wait_send()


def shards(depth_z, lower_coupling, upper_coupling, lower_inverse, upper_inverse, right_side):
    rows = right_side.shape[1]
    cols = right_side.shape[2] // 4
    quarter = rows // 4

    def split(a):
        return a.reshape(2, 2, 2, quarter, a.shape[2])

    f32, bf16 = jnp.float32, jnp.bfloat16
    dma = pltpu.SemaphoreType.DMA
    hbm = pl.BlockSpec(memory_space=pltpu.MemorySpace.HBM)
    return pl.pallas_call(
        functools.partial(kernel, depth_z),
        out_shape=jax.ShapeDtypeStruct(right_side.shape, f32),
        in_specs=[hbm] * 5,
        out_specs=pl.BlockSpec(memory_space=pltpu.MemorySpace.VMEM),
        scratch_shapes=[
            pltpu.VMEM((6, 4, 2, 2, quarter, 32 * rows), bf16),
            pltpu.VMEM((4, 4, 4, 2, rows, cols), bf16),
            pltpu.VMEM((2, 4, rows, cols), f32),
            pltpu.VMEM((4, rows, cols), bf16),
            pltpu.VMEM((4, rows, cols), f32),
            pltpu.VMEM((4 * rows, cols), f32),
            pltpu.VMEM((4 * rows, cols), f32),
            pltpu.VMEM((2, 4, rows, cols), bf16),
            pltpu.VMEM((2, 4, rows, cols), bf16),
            dma((4, 4)),
            dma((4, 13)), dma((4, 13)),
            dma((6, 10)), dma((6, 10)),
            dma((4,)), dma((4,)),
            dma((4,)), dma((4,)),
            dma((2, 4)), dma((2, 4)),
        ],
        compiler_params=pltpu.CompilerParams(
            collective_id=0, has_side_effects=True, vmem_limit_bytes=48 * 2**20
        ),
    )(split(lower_coupling), split(lower_inverse), split(upper_coupling), split(upper_inverse), right_side)


def solution(mesh):
    depth_z = mesh.shape["rhs"]
    finer = Mesh(mesh.devices.reshape(4, 4, 2, depth_z), BLK + ("rhs",))
    spec = P(None, BLK, None)
    return jax.shard_map(
        functools.partial(shards, depth_z),
        mesh=finer,
        in_specs=(spec, spec, spec, spec, P(None, BLK, "rhs")),
        out_specs=P(None, BLK, "rhs"),
        check_vma=False,
    )
```

```python
import functools

import jax
import jax.numpy as jnp
from jax import lax
from jax.experimental import pallas as pl
from jax.experimental.pallas import tpu as pltpu
from jax.sharding import Mesh
from jax.sharding import PartitionSpec as P

BLK = ("blk_0", "blk_1", "blk_2")
L10, LI1, U01, LI0, UI1, UI0 = range(6)
DIRECT = (True,) * 6
EARLY = (LI1, U01, LI0, UI1, UI0)


def kernel(
    depth_z, lc, li, uc, ui, b, o,
    w, v, bv, fst, b1g, acc, y0, ob, ro,
    hsem, ysend, yrecv, msend, mrecv, asend, arecv, bsend, brecv, xsend, xrecv,
):
    rows, cols = fst.shape[1], fst.shape[2]
    own = 4 * rows
    span = 2 * rows
    x, y, k, z = (lax.axis_index(a) for a in BLK + ("rhs",))
    xr, xl, xo = (x + 1) % 4, (x + 3) % 4, (x + 2) % 4
    yr, yl, yo = (y + 1) % 4, (y + 3) % 4, (y + 2) % 4
    zr, zl = (z + 1) % depth_z, (z + depth_z - 1) % depth_z
    p = z % 2
    q = 1 - p
    sib = 1 - k
    RIGHT, LEFT = (xr, y, k, z), (xl, y, k, z)
    UP, DOWN = (x, yr, k, z), (x, yl, k, z)
    NEXT, BACK = (x, y, k, zr), (x, y, k, zl)
    SIB = (x, y, sib, z)
    FAR = (xo, y, k, z)

    def remote(src, dst, ssem, rsem, dev):
        return pltpu.make_async_remote_copy(
            src_ref=src, dst_ref=dst, send_sem=ssem, recv_sem=rsem,
            device_id=dev, device_id_type=pl.DeviceIdType.MESH,
        )

    sent = []

    def send(src, sends, recvs, i, dev, dst=None):
        c = remote(src, src if dst is None else dst, sends.at[i], recvs.at[i], dev)
        c.start()
        sent.append(c)

    def arrived(ref, sends, recvs, i, dev):
        remote(ref, ref, sends.at[i], recvs.at[i], dev).wait_recv()

    barrier = pltpu.get_barrier_semaphore()
    greeted = [RIGHT, LEFT, FAR, UP, DOWN, SIB, NEXT, BACK]
    for dev in greeted:
        pl.semaphore_signal(barrier, inc=1, device_id=dev, device_id_type=pl.DeviceIdType.MESH)

    loads_b = [
        [
            pltpu.make_async_copy(b.at[s, :, c * cols:(c + 1) * cols], bv.at[s, c], hsem.at[s, c])
            for c in range(4)
        ]
        for s in range(2)
    ]
    sep = 32 * rows
    source = [
        lc.at[1, :, :, :, 0:sep], li.at[1], uc.at[0, :, :, :, sep:2 * sep],
        li.at[0], ui.at[1], ui.at[0],
    ]
    loads_w = [pltpu.make_async_copy(source[m], w.at[m, x], hsem.at[2 + m // 4, m % 4]) for m in range(6)]
    for c in loads_b[0]:
        c.start()
    loads_w[0].start()
    for c in loads_b[1]:
        c.start()
    for c in loads_w[1:]:
        c.start()
    for c in range(4):
        loads_b[0][c].wait()
        fst[c] = bv[0, c].astype(jnp.bfloat16)
    v[0, x, y, k] = fst[x]

    pl.semaphore_wait(barrier, len(greeted))

    def own_send(m):
        loads_w[m].wait()
        s, r = msend.at[m], mrecv.at[m]
        send(w.at[m, x, p], s, r, 0, RIGHT)
        send(w.at[m, x, p], s, r, 1, LEFT)
        if DIRECT[m]:
            send(w.at[m, x, p], s, r, 2, FAR)

    def own_later(m):
        if m not in EARLY:
            own_send(m)

    def relay(m):
        s, r = msend.at[m], mrecv.at[m]
        arrived(w.at[m, xl, p], s, r, 0, LEFT)
        if not DIRECT[m]:
            send(w.at[m, xl, p, 0], s, r, 2, RIGHT)
        send(w.at[m, xl, p, 0], s, r, 4, NEXT)
        send(w.at[m, xl, p, 1], s, r, 5, BACK)
        arrived(w.at[m, xr, p], s, r, 1, RIGHT)
        if not DIRECT[m]:
            send(w.at[m, xr, p, 1], s, r, 3, LEFT)
        send(w.at[m, xr, p, 0], s, r, 6, NEXT)
        send(w.at[m, xr, p, 1], s, r, 7, BACK)

    def relay_far(m):
        s, r = msend.at[m], mrecv.at[m]
        if DIRECT[m]:
            arrived(w.at[m, xo, p], s, r, 2, FAR)
        else:
            arrived(w.at[m, xo, p, 0], s, r, 2, LEFT)
        send(w.at[m, xo, p, 0], s, r, 8, NEXT)
        if not DIRECT[m]:
            arrived(w.at[m, xo, p, 1], s, r, 3, RIGHT)
        send(w.at[m, xo, p, 1], s, r, 9, BACK)

    def complete(m):
        s, r = msend.at[m], mrecv.at[m]
        for i, (src, part) in enumerate([(xl, 0), (xl, 1), (xr, 0), (xr, 1), (xo, 0), (xo, 1)]):
            arrived(w.at[m, src, q, part], s, r, 4 + i, BACK if part == 0 else NEXT)

    def product(m, s, yy):
        lhs = jnp.concatenate(
            [
                w[m, :, :, :, :, pl.ds(pl.multiple_of(c * 4 * span + yy * span, span), span)].reshape(own, span)
                for c in range(4)
            ],
            axis=1,
        )
        rhs = v[s, :, yy].reshape(4 * span, cols)
        return jnp.dot(lhs, rhs, preferred_element_type=jnp.float32)

    def full_product(m, s, dst):
        dst[...] = product(m, s, 0)
        for yy in range(1, 4):
            dst[...] += product(m, s, yy)

    def gather(s, m, start=None, near=None, second=None, far=None, ready=None):
        ss, rr = ysend.at[s], yrecv.at[s]
        send(v.at[s, 0:2, y, k], ss, rr, 0, UP)
        send(v.at[s, 2:4, y, k], ss, rr, 2, DOWN)
        send(v.at[s, 2:4, y, k], ss, rr, 1, UP)
        send(v.at[s, 0:2, y, k], ss, rr, 3, DOWN)
        send(v.at[s, :, y, k], ss, rr, 6, SIB)
        if start is not None:
            start()
        arrived(v.at[s, 0:2, yl, k], ss, rr, 0, DOWN)
        send(v.at[s, 0:2, yl, k], ss, rr, 4, UP)
        send(v.at[s, 0:2, yl, k], ss, rr, 7, SIB)
        arrived(v.at[s, 2:4, yr, k], ss, rr, 2, UP)
        send(v.at[s, 2:4, yr, k], ss, rr, 5, DOWN)
        send(v.at[s, 2:4, yr, k], ss, rr, 9, SIB)
        if near is not None:
            near()
        arrived(v.at[s, 2:4, yl, k], ss, rr, 1, DOWN)
        send(v.at[s, 2:4, yl, k], ss, rr, 8, SIB)
        arrived(v.at[s, 0:2, yr, k], ss, rr, 3, UP)
        send(v.at[s, 0:2, yr, k], ss, rr, 10, SIB)
        if second is not None:
            second()

        def first_product():
            arrived(v.at[s, :, y, sib], ss, rr, 6, SIB)
            acc[...] = product(m, s, y)

        def near_products():
            arrived(v.at[s, 0:2, yl, sib], ss, rr, 7, SIB)
            arrived(v.at[s, 2:4, yl, sib], ss, rr, 8, SIB)
            acc[...] += product(m, s, yl)
            arrived(v.at[s, 2:4, yr, sib], ss, rr, 9, SIB)
            arrived(v.at[s, 0:2, yr, sib], ss, rr, 10, SIB)
            acc[...] += product(m, s, yr)

        if ready is None:
            first_product()
            near_products()
        arrived(v.at[s, 0:2, yo, k], ss, rr, 4, DOWN)
        send(v.at[s, 0:2, yo, k], ss, rr, 11, SIB)
        arrived(v.at[s, 2:4, yo, k], ss, rr, 5, UP)
        send(v.at[s, 2:4, yo, k], ss, rr, 12, SIB)
        if far is not None:
            far()
        if ready is not None:
            ready()
            first_product()
            near_products()
        arrived(v.at[s, 0:2, yo, sib], ss, rr, 11, SIB)
        arrived(v.at[s, 2:4, yo, sib], ss, rr, 12, SIB)
        acc[...] += product(m, s, yo)

    def result(s, total):
        ob[s] = total[...].reshape(4, rows, cols).astype(jnp.bfloat16)
        for d in (2, 1, 3):
            send(ob.at[s, (x + d) % 4], xsend.at[s], xrecv.at[s], d, ((x + d) % 4, y, k, z), ro.at[s, x])

    def write(s):
        ro[s, x] = ob[s, x]
        for d in (1, 3, 2):
            arrived(ro.at[s, (x + 4 - d) % 4], xsend.at[s], xrecv.at[s], d, ((x + 4 - d) % 4, y, k, z))
        for c in range(4):
            o[s, :, c * cols:(c + 1) * cols] = ro[s, c].astype(jnp.float32)

    def residual(s, values):
        v[s, :, y, k] = values.astype(jnp.bfloat16).reshape(4, rows, cols)

    def in_turn(*steps):
        def run():
            for step in steps:
                step()
        return run

    def do(step, *args):
        return functools.partial(step, *args)

    for d in (1, 3, 2):
        send(fst.at[(x + d) % 4], asend, arecv, d, ((x + d) % 4, y, k, z), v.at[0, x, y, k])
    own_send(L10)
    for c in loads_b[1]:
        c.wait()
    b1g[x] = bv[1, x]
    for d in (1, 3, 2):
        send(bv.at[1, (x + d) % 4], bsend, brecv, d, ((x + d) % 4, y, k, z), b1g.at[x])
    for m in EARLY:
        own_send(m)
    for d in (1, 3, 2):
        arrived(v.at[0, (x + 4 - d) % 4, y, k], asend, arecv, d, ((x + 4 - d) % 4, y, k, z))
    gather(
        0, L10,
        start=do(relay, L10),
        near=in_turn(do(relay_far, L10), do(own_later, U01)),
        ready=do(complete, L10),
    )
    for d in (1, 3, 2):
        arrived(b1g.at[(x + 4 - d) % 4], bsend, brecv, d, ((x + 4 - d) % 4, y, k, z))

    residual(1, b1g[...].reshape(own, cols) - acc[...])
    gather(
        1, LI1,
        start=in_turn(do(relay, LI1), do(own_later, LI0)),
        second=in_turn(do(relay_far, LI1), do(own_later, UI1)),
        far=do(relay, U01),
        ready=do(complete, LI1),
    )

    residual(2, acc[...])
    gather(
        2, U01,
        start=do(relay_far, U01),
        near=in_turn(do(relay, LI0), do(own_later, UI0)),
        second=do(complete, U01),
        far=in_turn(do(relay_far, LI0), do(complete, LI0), do(full_product, LI0, 0, y0)),
    )

    residual(3, y0[...] - acc[...])

    def other_result():
        complete(UI1)
        full_product(UI1, 2, y0)
        result(1, y0)

    gather(
        3, UI0,
        start=do(relay, UI1),
        near=do(relay_far, UI1),
        second=do(relay, UI0),
        far=do(relay_far, UI0),
        ready=in_turn(other_result, do(complete, UI0)),
    )
    result(0, acc)
    write(1)
    write(0)
    for c in sent:
        c.wait_send()


def shards(depth_z, lower_coupling, upper_coupling, lower_inverse, upper_inverse, right_side):
    rows = right_side.shape[1]
    cols = right_side.shape[2] // 4
    quarter = rows // 4

    def split(a):
        return a.reshape(2, 2, 2, quarter, a.shape[2])

    f32, bf16 = jnp.float32, jnp.bfloat16
    dma = pltpu.SemaphoreType.DMA
    hbm = pl.BlockSpec(memory_space=pltpu.MemorySpace.HBM)
    return pl.pallas_call(
        functools.partial(kernel, depth_z),
        out_shape=jax.ShapeDtypeStruct(right_side.shape, f32),
        in_specs=[hbm] * 5,
        out_specs=pl.BlockSpec(memory_space=pltpu.MemorySpace.VMEM),
        scratch_shapes=[
            pltpu.VMEM((6, 4, 2, 2, quarter, 32 * rows), bf16),
            pltpu.VMEM((4, 4, 4, 2, rows, cols), bf16),
            pltpu.VMEM((2, 4, rows, cols), f32),
            pltpu.VMEM((4, rows, cols), bf16),
            pltpu.VMEM((4, rows, cols), f32),
            pltpu.VMEM((4 * rows, cols), f32),
            pltpu.VMEM((4 * rows, cols), f32),
            pltpu.VMEM((2, 4, rows, cols), bf16),
            pltpu.VMEM((2, 4, rows, cols), bf16),
            dma((4, 4)),
            dma((4, 13)), dma((4, 13)),
            dma((6, 10)), dma((6, 10)),
            dma((4,)), dma((4,)),
            dma((4,)), dma((4,)),
            dma((2, 4)), dma((2, 4)),
        ],
        compiler_params=pltpu.CompilerParams(
            collective_id=0, has_side_effects=True, vmem_limit_bytes=53 * 2**20
        ),
    )(split(lower_coupling), split(lower_inverse), split(upper_coupling), split(upper_inverse), right_side)


def solution(mesh):
    depth_z = mesh.shape["rhs"]
    finer = Mesh(mesh.devices.reshape(4, 4, 2, depth_z), BLK + ("rhs",))
    spec = P(None, BLK, None)
    return jax.shard_map(
        functools.partial(shards, depth_z),
        mesh=finer,
        in_specs=(spec, spec, spec, spec, P(None, BLK, "rhs")),
        out_specs=P(None, BLK, "rhs"),
        check_vma=False,
    )
```

```python
import functools

import jax
import jax.numpy as jnp
from jax import lax
from jax.experimental import pallas as pl
from jax.experimental.pallas import tpu as pltpu
from jax.sharding import Mesh
from jax.sharding import PartitionSpec as P

BLK = ("blk_0", "blk_1", "blk_2")
L10, LI1, U01, LI0, UI1, UI0 = range(6)
CHUNKS = 2


def kernel(
    lc, li, uc, ui, b, o,
    w, v, bv, fst, b1g, y0, ob, ro,
    hsem, vsend, vrecv, msend, mrecv, asend, arecv, bsend, brecv, xsend, xrecv,
):
    rows, width = fst.shape[3], fst.shape[4]
    cols = CHUNKS * width
    own = 4 * rows
    x, y, k, z = (lax.axis_index(a) for a in BLK + ("rhs",))
    t = x // 2
    j = t * (3 - x) + (1 - t) * x
    i = 1 - j
    u = 1 - t
    n = 1 - k
    yr, yl, yo = (y + 1) % 4, (y + 3) % 4, (y + 2) % 4
    SIDE = (x + 1 - 2 * (x % 2), y, k, z)
    PAIR, CROSS, SIB = (3 - x, y, k, z), (3 - x, y, n, z), (x, y, n, z)
    UP, DOWN, FAR = (x, yr, k, z), (x, yl, k, z), (x, yo, k, z)

    def remote(src, dst, ssem, rsem, dev):
        return pltpu.make_async_remote_copy(
            src_ref=src, dst_ref=dst, send_sem=ssem, recv_sem=rsem,
            device_id=dev, device_id_type=pl.DeviceIdType.MESH,
        )

    sent = []

    def send(src, sends, recvs, dev, dst=None):
        c = remote(src, src if dst is None else dst, sends, recvs, dev)
        c.start()
        sent.append(c)

    def arrived(ref, sends, recvs, dev):
        remote(ref, ref, sends, recvs, dev).wait_recv()

    barrier = pltpu.get_barrier_semaphore()
    greeted = [SIDE, PAIR, CROSS, SIB, UP, DOWN, FAR]
    for dev in greeted:
        pl.semaphore_signal(barrier, inc=1, device_id=dev, device_id_type=pl.DeviceIdType.MESH)

    def load_b(s, half, core):
        first = (half * 2 + core) * cols
        return pltpu.make_async_copy(
            b.at[s, :, first:first + cols], bv.at[s, half, core], hsem.at[s, half * 2 + core]
        )

    loads_b = [[load_b(s, half, core) for half in range(2) for core in range(2)] for s in range(2)]
    sep = 32 * rows
    source = [
        lc.at[1, :, 0:sep], li.at[1], uc.at[0, :, sep:2 * sep], li.at[0], ui.at[1], ui.at[0],
    ]
    loads_w = [
        pltpu.make_async_copy(source[m], w.at[m, t, k], hsem.at[2 + m // 4, m % 4]) for m in range(6)
    ]
    for c in loads_b[0]:
        c.start()
    loads_w[0].start()
    for c in loads_b[1]:
        c.start()
    for c in loads_w[1:]:
        c.start()
    for half in range(2):
        for core in range(2):
            loads_b[0][half * 2 + core].wait()
            for c in range(CHUNKS):
                fst[half, core, c] = bv[0, half, core, :, c * width:(c + 1) * width].astype(jnp.bfloat16)
    for c in range(CHUNKS):
        v[0, c, j, t, y, k] = fst[t, k, c]

    pl.semaphore_wait(barrier, len(greeted))

    def own_send(m):
        loads_w[m].wait()
        send(w.at[m, t, k], msend.at[m, 0], mrecv.at[m, 0], PAIR)
        send(w.at[m, t, k], msend.at[m, 1], mrecv.at[m, 1], SIB)

    def pass_on(m):
        arrived(w.at[m, u, k], msend.at[m, 0], mrecv.at[m, 0], PAIR)
        send(w.at[m, u, k], msend.at[m, 2], mrecv.at[m, 2], SIB)

    def complete(m):
        arrived(w.at[m, t, n], msend.at[m, 1], mrecv.at[m, 1], SIB)
        arrived(w.at[m, u, n], msend.at[m, 2], mrecv.at[m, 2], SIB)

    def product(m, s, c):
        total = None
        for jj in range(2):
            for h in range(2):
                first = (jj if h == 0 else 3 - jj) * 8 * rows
                lhs = w[m, :, :, :, first:first + 8 * rows].reshape(own, 8 * rows)
                rhs = v[s, c, jj, h].reshape(8 * rows, width)
                part = jnp.dot(lhs, rhs, preferred_element_type=jnp.float32)
                total = part if total is None else total + part
        return total

    def spread(s, c):
        ss, rr = vsend.at[s, c], vrecv.at[s, c]
        mine = v.at[s, c, j, :, y]
        send(mine, ss.at[0], rr.at[0], FAR)
        send(mine, ss.at[1], rr.at[1], SIDE)
        send(mine, ss.at[2], rr.at[2], UP)
        send(mine, ss.at[3], rr.at[3], DOWN)

    def relay(s, c):
        ss, rr = vsend.at[s, c], vrecv.at[s, c]
        side, far = v.at[s, c, i, :, y], v.at[s, c, j, :, yo]
        arrived(side, ss.at[1], rr.at[1], SIDE)
        send(side, ss.at[5], rr.at[5], UP)
        send(side, ss.at[6], rr.at[6], DOWN)
        arrived(far, ss.at[0], rr.at[0], FAR)
        send(far, ss.at[4], rr.at[4], SIDE)

    def gathered(s, c):
        ss, rr = vsend.at[s, c], vrecv.at[s, c]
        arrived(v.at[s, c, j, :, yl], ss.at[2], rr.at[2], DOWN)
        arrived(v.at[s, c, j, :, yr], ss.at[3], rr.at[3], UP)
        arrived(v.at[s, c, i, :, yl], ss.at[5], rr.at[5], DOWN)
        arrived(v.at[s, c, i, :, yr], ss.at[6], rr.at[6], UP)
        arrived(v.at[s, c, i, :, yo], ss.at[4], rr.at[4], SIDE)

    def residual(s, c, values):
        v[s, c, j, :, y] = values.astype(jnp.bfloat16).reshape(2, 2, rows, width)
        spread(s, c)

    def result(s, c, total):
        ob[s, c] = total.astype(jnp.bfloat16).reshape(2, 2, rows, width)
        ss, rr = xsend.at[s, c], xrecv.at[s, c]
        send(ob.at[s, c, u, k], ss.at[0], rr.at[0], PAIR, ro.at[s, c, t, k])
        send(ob.at[s, c, u, n], ss.at[1], rr.at[1], CROSS, ro.at[s, c, t, k])
        send(ob.at[s, c, t, n], ss.at[2], rr.at[2], SIB, ro.at[s, c, t, k])
        ro[s, c, t, k] = ob[s, c, t, k]

    def write(s, c):
        ss, rr = xsend.at[s, c], xrecv.at[s, c]
        arrived(ro.at[s, c, t, n], ss.at[2], rr.at[2], SIB)
        arrived(ro.at[s, c, u, k], ss.at[0], rr.at[0], PAIR)
        arrived(ro.at[s, c, u, n], ss.at[1], rr.at[1], CROSS)
        for half in range(2):
            for core in range(2):
                first = (half * 2 + core) * cols + c * width
                o[s, :, first:first + width] = ro[s, c, half, core].astype(jnp.float32)

    every = range(CHUNKS)
    for c in every:
        send(fst.at[u, k, c], asend.at[c, 0], arecv.at[c, 0], PAIR, v.at[0, c, j, t, y, k])
        send(fst.at[u, n, c], asend.at[c, 1], arecv.at[c, 1], CROSS, v.at[0, c, j, t, y, k])
        send(fst.at[t, n, c], asend.at[c, 2], arecv.at[c, 2], SIB, v.at[0, c, j, t, y, k])
    own_send(L10)
    for c in loads_b[1]:
        c.wait()
    send(bv.at[1, u, k], bsend.at[0], brecv.at[0], PAIR, b1g.at[t, k])
    send(bv.at[1, u, n], bsend.at[1], brecv.at[1], CROSS, b1g.at[t, k])
    send(bv.at[1, t, n], bsend.at[2], brecv.at[2], SIB, b1g.at[t, k])
    for m in range(1, 6):
        own_send(m)
    b1g[t, k] = bv[1, t, k]
    for c in every:
        arrived(v.at[0, c, j, t, y, n], asend.at[c, 2], arecv.at[c, 2], SIB)
        arrived(v.at[0, c, j, u, y, k], asend.at[c, 0], arecv.at[c, 0], PAIR)
        arrived(v.at[0, c, j, u, y, n], asend.at[c, 1], arecv.at[c, 1], CROSS)
        spread(0, c)
    for c in every:
        relay(0, c)
    pass_on(L10)
    arrived(b1g.at[t, n], bsend.at[2], brecv.at[2], SIB)
    arrived(b1g.at[u, k], bsend.at[0], brecv.at[0], PAIR)
    arrived(b1g.at[u, n], bsend.at[1], brecv.at[1], CROSS)
    complete(L10)
    for c in every:
        gathered(0, c)
        start = b1g[:, :, :, c * width:(c + 1) * width].reshape(own, width)
        residual(1, c, start - product(L10, 0, c))
    for c in every:
        relay(1, c)
    pass_on(LI1)
    complete(LI1)
    for c in every:
        gathered(1, c)
        residual(2, c, product(LI1, 1, c))
    pass_on(U01)
    for c in every:
        relay(2, c)
    complete(U01)
    pass_on(LI0)
    complete(LI0)
    for c in every:
        y0[c] = product(LI0, 0, c)
    for c in every:
        gathered(2, c)
        residual(3, c, y0[c] - product(U01, 2, c))
    pass_on(UI1)
    for c in every:
        relay(3, c)
    complete(UI1)
    for c in every:
        result(1, c, product(UI1, 2, c))
    pass_on(UI0)
    complete(UI0)
    for c in every:
        gathered(3, c)
        result(0, c, product(UI0, 3, c))
    for s in (1, 0):
        for c in every:
            write(s, c)
    for c in sent:
        c.wait_send()


def shards(lower_coupling, upper_coupling, lower_inverse, upper_inverse, right_side):
    rows = right_side.shape[1]
    cols = right_side.shape[2] // 4
    width = cols // CHUNKS
    f32, bf16 = jnp.float32, jnp.bfloat16
    dma = pltpu.SemaphoreType.DMA
    hbm = pl.BlockSpec(memory_space=pltpu.MemorySpace.HBM)
    return pl.pallas_call(
        kernel,
        out_shape=jax.ShapeDtypeStruct(right_side.shape, f32),
        in_specs=[hbm] * 5,
        out_specs=pl.BlockSpec(memory_space=pltpu.MemorySpace.VMEM),
        scratch_shapes=[
            pltpu.VMEM((6, 2, 2, rows, 32 * rows), bf16),
            pltpu.VMEM((4, CHUNKS, 2, 2, 4, 2, rows, width), bf16),
            pltpu.VMEM((2, 2, 2, rows, cols), f32),
            pltpu.VMEM((2, 2, CHUNKS, rows, width), bf16),
            pltpu.VMEM((2, 2, rows, cols), f32),
            pltpu.VMEM((CHUNKS, 4 * rows, width), f32),
            pltpu.VMEM((2, CHUNKS, 2, 2, rows, width), bf16),
            pltpu.VMEM((2, CHUNKS, 2, 2, rows, width), bf16),
            dma((4, 4)),
            dma((4, CHUNKS, 7)), dma((4, CHUNKS, 7)),
            dma((6, 3)), dma((6, 3)),
            dma((CHUNKS, 3)), dma((CHUNKS, 3)),
            dma((3,)), dma((3,)),
            dma((2, CHUNKS, 3)), dma((2, CHUNKS, 3)),
        ],
        compiler_params=pltpu.CompilerParams(
            collective_id=0, has_side_effects=True, vmem_limit_bytes=53 * 2**20
        ),
    )(lower_coupling, lower_inverse, upper_coupling, upper_inverse, right_side)


def solution(mesh):
    finer = Mesh(mesh.devices.reshape(4, 4, 2, mesh.shape["rhs"]), BLK + ("rhs",))
    spec = P(None, BLK, None)
    return jax.shard_map(
        shards,
        mesh=finer,
        in_specs=(spec, spec, spec, spec, P(None, BLK, "rhs")),
        out_specs=P(None, BLK, "rhs"),
        check_vma=False,
    )
```

```python
import functools

import jax
import jax.numpy as jnp
from jax import lax
from jax.experimental import pallas as pl
from jax.experimental.pallas import tpu as pltpu
from jax.sharding import Mesh
from jax.sharding import PartitionSpec as P

BLK = ("blk_0", "blk_1", "blk_2")
L10, LI1, LI0, U01, UI1, UI0 = range(6)
CHUNKS = 2


def kernel(
    lc, li, uc, ui, b, o,
    w, v, bv, fst, b1g, y0, ob, ro,
    hsem, vsend, vrecv, msend, mrecv, asend, arecv, bsend, brecv, xsend, xrecv,
):
    rows, width = fst.shape[3], fst.shape[4]
    cols = CHUNKS * width
    own = 4 * rows
    x, y, k, z = (lax.axis_index(a) for a in BLK + ("rhs",))
    t = x // 2
    j = t * (3 - x) + (1 - t) * x
    i = 1 - j
    u = 1 - t
    n = 1 - k
    yr, yl, yo = (y + 1) % 4, (y + 3) % 4, (y + 2) % 4
    SIDE = (x + 1 - 2 * (x % 2), y, k, z)
    PAIR, CROSS, SIB = (3 - x, y, k, z), (3 - x, y, n, z), (x, y, n, z)
    UP, DOWN, FAR = (x, yr, k, z), (x, yl, k, z), (x, yo, k, z)

    def remote(src, dst, ssem, rsem, dev):
        return pltpu.make_async_remote_copy(
            src_ref=src, dst_ref=dst, send_sem=ssem, recv_sem=rsem,
            device_id=dev, device_id_type=pl.DeviceIdType.MESH,
        )

    sent = []

    def send(src, sends, recvs, dev, dst=None):
        c = remote(src, src if dst is None else dst, sends, recvs, dev)
        c.start()
        sent.append(c)

    def arrived(ref, sends, recvs, dev):
        remote(ref, ref, sends, recvs, dev).wait_recv()

    barrier = pltpu.get_barrier_semaphore()
    greeted = [SIDE, PAIR, CROSS, SIB, UP, DOWN, FAR]
    for dev in greeted:
        pl.semaphore_signal(barrier, inc=1, device_id=dev, device_id_type=pl.DeviceIdType.MESH)

    def load_b(s, half, core, c):
        first = (half * 2 + core) * cols + c * width
        return pltpu.make_async_copy(
            b.at[s, :, first:first + width], bv.at[s, half, core, c],
            hsem.at[s, (half * 2 + core) * CHUNKS + c],
        )

    pieces = [(half, core, c) for half in range(2) for core in range(2) for c in range(CHUNKS)]
    loads_b = [[load_b(s, *piece) for piece in pieces] for s in range(2)]
    sep = 32 * rows
    source = [
        lc.at[1, :, 0:sep], li.at[1], li.at[0], uc.at[0, :, sep:2 * sep], ui.at[1], ui.at[0],
    ]
    loads_w = [
        pltpu.make_async_copy(source[m], w.at[m, t, k], hsem.at[2, m]) for m in range(6)
    ]
    for c in loads_b[0]:
        c.start()
    loads_w[0].start()
    for c in loads_b[1]:
        c.start()
    for c in loads_w[1:]:
        c.start()
    for piece, load in zip(pieces, loads_b[0]):
        load.wait()
        fst[piece] = bv[(0,) + piece].astype(jnp.bfloat16)
    for c in range(CHUNKS):
        v[0, c, j, t, y, k] = fst[t, k, c]

    pl.semaphore_wait(barrier, len(greeted))

    def own_send(m):
        loads_w[m].wait()
        send(w.at[m, t, k], msend.at[m, 0], mrecv.at[m, 0], PAIR)
        send(w.at[m, t, k], msend.at[m, 1], mrecv.at[m, 1], SIB)

    def pass_on(m):
        arrived(w.at[m, u, k], msend.at[m, 0], mrecv.at[m, 0], PAIR)
        send(w.at[m, u, k], msend.at[m, 2], mrecv.at[m, 2], SIB)

    def own_complete(m):
        arrived(w.at[m, t, n], msend.at[m, 1], mrecv.at[m, 1], SIB)

    def pair_complete(m):
        arrived(w.at[m, u, n], msend.at[m, 2], mrecv.at[m, 2], SIB)

    def complete(m):
        own_complete(m)
        pair_complete(m)

    def rows_of(chip, m, s, c):
        total = None
        for jj in range(2):
            for h in range(2):
                first = (jj if h == 0 else 3 - jj) * 8 * rows
                lhs = w[m, chip, :, :, first:first + 8 * rows]
                rhs = v[s, c, jj, h].reshape(8 * rows, width)
                part = jnp.dot(lhs.reshape(-1, 8 * rows), rhs, preferred_element_type=jnp.float32)
                total = part if total is None else total + part
        return total

    def product(m, s, c):
        return rows_of(slice(None), m, s, c)

    def near(s, c, e, h):
        ss, rr = vsend.at[s, c], vrecv.at[s, c]
        send(v.at[s, c, j, h, y], ss.at[2, e], rr.at[2, e], UP)
        send(v.at[s, c, j, h, y], ss.at[3, e], rr.at[3, e], DOWN)

    def spread(s, c, halves):
        ss, rr = vsend.at[s, c], vrecv.at[s, c]
        for e, h in halves:
            send(v.at[s, c, j, h, y], ss.at[0, e], rr.at[0, e], FAR)
            send(v.at[s, c, j, h, y], ss.at[1, e], rr.at[1, e], SIDE)
        if halves[0][0] == 0:
            near(s, c, *halves[0])

    def relay(s, c, halves):
        ss, rr = vsend.at[s, c], vrecv.at[s, c]
        for e, h in halves:
            side = v.at[s, c, i, h, y]
            arrived(side, ss.at[1, e], rr.at[1, e], SIDE)
            if e == 0:
                near(s, c, *halves[1])
            send(side, ss.at[5, e], rr.at[5, e], UP)
            send(side, ss.at[6, e], rr.at[6, e], DOWN)
        for e, h in halves:
            far = v.at[s, c, j, h, yo]
            arrived(far, ss.at[0, e], rr.at[0, e], FAR)
            send(far, ss.at[4, e], rr.at[4, e], SIDE)

    def gathered(s, c, halves):
        ss, rr = vsend.at[s, c], vrecv.at[s, c]
        for e, h in halves:
            arrived(v.at[s, c, j, h, yl], ss.at[2, e], rr.at[2, e], DOWN)
            arrived(v.at[s, c, i, h, yl], ss.at[5, e], rr.at[5, e], DOWN)
            arrived(v.at[s, c, j, h, yr], ss.at[3, e], rr.at[3, e], UP)
            arrived(v.at[s, c, i, h, yr], ss.at[6, e], rr.at[6, e], UP)
            arrived(v.at[s, c, i, h, yo], ss.at[4, e], rr.at[4, e], SIDE)

    def residual(s, c, values):
        v[s, c, j, :, y] = values.astype(jnp.bfloat16).reshape(2, 2, rows, width)
        spread(s, c, plain)

    def result_own(s, c, total):
        ob[s, c, t] = total.astype(jnp.bfloat16).reshape(2, rows, width)
        send(ob.at[s, c, t, n], xsend.at[s, c, 2], xrecv.at[s, c, 2], SIB, ro.at[s, c, t, k])
        ro[s, c, t, k] = ob[s, c, t, k]

    def result_pair(s, c, total):
        ob[s, c, u] = total.astype(jnp.bfloat16).reshape(2, rows, width)
        send(ob.at[s, c, u, k], xsend.at[s, c, 0], xrecv.at[s, c, 0], PAIR, ro.at[s, c, t, k])
        send(ob.at[s, c, u, n], xsend.at[s, c, 1], xrecv.at[s, c, 1], CROSS, ro.at[s, c, t, k])

    def write(s, c):
        ss, rr = xsend.at[s, c], xrecv.at[s, c]
        arrived(ro.at[s, c, t, n], ss.at[2], rr.at[2], SIB)
        arrived(ro.at[s, c, u, k], ss.at[0], rr.at[0], PAIR)
        arrived(ro.at[s, c, u, n], ss.at[1], rr.at[1], CROSS)
        for half in range(2):
            for core in range(2):
                first = (half * 2 + core) * cols + c * width
                o[s, :, first:first + width] = ro[s, c, half, core].astype(jnp.float32)

    every = range(CHUNKS)

    def relays(s, halves):
        for c in every:
            relay(s, c, halves)

    for c in every:
        send(fst.at[u, k, c], asend.at[c, 0], arecv.at[c, 0], PAIR, v.at[0, c, j, t, y, k])
        send(fst.at[u, n, c], asend.at[c, 1], arecv.at[c, 1], CROSS, v.at[0, c, j, t, y, k])
        send(fst.at[t, n, c], asend.at[c, 2], arecv.at[c, 2], SIB, v.at[0, c, j, t, y, k])
    own_send(L10)
    for c in loads_b[1]:
        c.wait()
    for c in every:
        send(bv.at[1, u, k, c], bsend.at[c, 0], brecv.at[c, 0], PAIR, b1g.at[c, t, k])
        send(bv.at[1, u, n, c], bsend.at[c, 1], brecv.at[c, 1], CROSS, b1g.at[c, t, k])
        send(bv.at[1, t, n, c], bsend.at[c, 2], brecv.at[c, 2], SIB, b1g.at[c, t, k])
    for m in range(1, 6):
        own_send(m)
    for c in every:
        b1g[c, t, k] = bv[1, t, k, c]
    plain, mine_first = ((0, 0), (1, 1)), ((0, t), (1, u))
    for c in every:
        arrived(v.at[0, c, j, t, y, n], asend.at[c, 2], arecv.at[c, 2], SIB)
        spread(0, c, mine_first[:1])
    for c in every:
        arrived(v.at[0, c, j, u, y, k], asend.at[c, 0], arecv.at[c, 0], PAIR)
        arrived(v.at[0, c, j, u, y, n], asend.at[c, 1], arecv.at[c, 1], CROSS)
        spread(0, c, mine_first[1:])
    relays(0, mine_first)
    pass_on(L10)
    complete(L10)
    for c in every:
        gathered(0, c, mine_first)
        arrived(b1g.at[c, t, n], bsend.at[c, 2], brecv.at[c, 2], SIB)
        arrived(b1g.at[c, u, k], bsend.at[c, 0], brecv.at[c, 0], PAIR)
        arrived(b1g.at[c, u, n], bsend.at[c, 1], brecv.at[c, 1], CROSS)
        start = b1g[c].reshape(own, width)
        residual(1, c, start - product(L10, 0, c))
    relays(1, plain)
    pass_on(LI1)
    complete(LI1)
    for c in every:
        gathered(1, c, plain)
        residual(2, c, product(LI1, 1, c))
    pass_on(LI0)
    relays(2, plain)
    complete(LI0)
    pass_on(U01)
    for c in every:
        y0[c] = product(LI0, 0, c)
    complete(U01)
    for c in every:
        gathered(2, c, plain)
        residual(3, c, y0[c] - product(U01, 2, c))
    pass_on(UI1)
    relays(3, plain)
    own_complete(UI1)
    for c in every:
        result_own(1, c, rows_of(t, UI1, 2, c))
    pair_complete(UI1)
    for c in every:
        result_pair(1, c, rows_of(u, UI1, 2, c))
    own_complete(UI0)
    gathered(3, 0, plain)
    result_own(0, 0, rows_of(t, UI0, 3, 0))
    pass_on(UI0)
    gathered(3, 1, plain)
    result_own(0, 1, rows_of(t, UI0, 3, 1))
    pair_complete(UI0)
    for c in every:
        result_pair(0, c, rows_of(u, UI0, 3, c))
    for s in (1, 0):
        for c in every:
            write(s, c)
    for c in sent:
        c.wait_send()


def shards(lower_coupling, upper_coupling, lower_inverse, upper_inverse, right_side):
    rows = right_side.shape[1]
    cols = right_side.shape[2] // 4
    width = cols // CHUNKS
    f32, bf16 = jnp.float32, jnp.bfloat16
    dma = pltpu.SemaphoreType.DMA
    hbm = pl.BlockSpec(memory_space=pltpu.MemorySpace.HBM)
    return pl.pallas_call(
        kernel,
        out_shape=jax.ShapeDtypeStruct(right_side.shape, f32),
        in_specs=[hbm] * 5,
        out_specs=pl.BlockSpec(memory_space=pltpu.MemorySpace.VMEM),
        scratch_shapes=[
            pltpu.VMEM((6, 2, 2, rows, 32 * rows), bf16),
            pltpu.VMEM((4, CHUNKS, 2, 2, 4, 2, rows, width), bf16),
            pltpu.VMEM((2, 2, 2, CHUNKS, rows, width), f32),
            pltpu.VMEM((2, 2, CHUNKS, rows, width), bf16),
            pltpu.VMEM((CHUNKS, 2, 2, rows, width), f32),
            pltpu.VMEM((CHUNKS, 4 * rows, width), f32),
            pltpu.VMEM((2, CHUNKS, 2, 2, rows, width), bf16),
            pltpu.VMEM((2, CHUNKS, 2, 2, rows, width), bf16),
            dma((3, 8)),
            dma((4, CHUNKS, 7, 2)), dma((4, CHUNKS, 7, 2)),
            dma((6, 3)), dma((6, 3)),
            dma((CHUNKS, 3)), dma((CHUNKS, 3)),
            dma((CHUNKS, 3)), dma((CHUNKS, 3)),
            dma((2, CHUNKS, 3)), dma((2, CHUNKS, 3)),
        ],
        compiler_params=pltpu.CompilerParams(
            collective_id=0, has_side_effects=True, vmem_limit_bytes=53 * 2**20
        ),
    )(lower_coupling, lower_inverse, upper_coupling, upper_inverse, right_side)


def solution(mesh):
    finer = Mesh(mesh.devices.reshape(4, 4, 2, mesh.shape["rhs"]), BLK + ("rhs",))
    spec = P(None, BLK, None)
    return jax.shard_map(
        shards,
        mesh=finer,
        in_specs=(spec, spec, spec, spec, P(None, BLK, "rhs")),
        out_specs=P(None, BLK, "rhs"),
        check_vma=False,
    )
```

```python
import functools

import jax
import jax.numpy as jnp
from jax import lax
from jax.experimental import pallas as pl
from jax.experimental.pallas import tpu as pltpu
from jax.sharding import Mesh
from jax.sharding import PartitionSpec as P

BLK = ("blk_0", "blk_1", "blk_2")
L10, LI1, LI0, U01, UI1, UI0 = range(6)
CHUNKS = 2


def kernel(
    lc, li, uc, ui, b, o,
    w, v, bv, fst, b1g, y0, ob, ro,
    hsem, vsend, vrecv, msend, mrecv, asend, arecv, bsend, brecv, xsend, xrecv,
):
    rows, width = fst.shape[3], fst.shape[4]
    cols = CHUNKS * width
    own = 4 * rows
    x, y, k, z = (lax.axis_index(a) for a in BLK + ("rhs",))
    t = ((x + 1) // 2) % 2
    j = x // 2
    i = 1 - j
    u = 1 - t
    n = 1 - k
    yr, yl, yo = (y + 1) % 4, (y + 3) % 4, (y + 2) % 4
    xp = x + 1 - 2 * (x % 2)
    SIDE = (3 - x, y, k, z)
    PAIR, CROSS, SIB = (xp, y, k, z), (xp, y, n, z), (x, y, n, z)
    UP, DOWN, FAR = (x, yr, k, z), (x, yl, k, z), (x, yo, k, z)

    def remote(src, dst, ssem, rsem, dev):
        return pltpu.make_async_remote_copy(
            src_ref=src, dst_ref=dst, send_sem=ssem, recv_sem=rsem,
            device_id=dev, device_id_type=pl.DeviceIdType.MESH,
        )

    sent = []

    def send(src, sends, recvs, dev, dst=None):
        c = remote(src, src if dst is None else dst, sends, recvs, dev)
        c.start()
        sent.append(c)

    def arrived(ref, sends, recvs, dev):
        remote(ref, ref, sends, recvs, dev).wait_recv()

    barrier = pltpu.get_barrier_semaphore()
    greeted = [SIDE, PAIR, CROSS, SIB, UP, DOWN, FAR]
    for dev in greeted:
        pl.semaphore_signal(barrier, inc=1, device_id=dev, device_id_type=pl.DeviceIdType.MESH)

    def load_b(s, half, core, c):
        first = (half * 2 + core) * cols + c * width
        return pltpu.make_async_copy(
            b.at[s, :, first:first + width], bv.at[s, half, core, c],
            hsem.at[s, (half * 2 + core) * CHUNKS + c],
        )

    pieces = [(half, core, c) for half in range(2) for core in range(2) for c in range(CHUNKS)]
    loads_b = [[load_b(s, *piece) for piece in pieces] for s in range(2)]
    sep = 32 * rows
    source = [
        lc.at[1, :, 0:sep], li.at[1], li.at[0], uc.at[0, :, sep:2 * sep], ui.at[1], ui.at[0],
    ]
    loads_w = [
        pltpu.make_async_copy(source[m], w.at[m, t, k], hsem.at[2, m]) for m in range(6)
    ]
    for c in loads_b[0]:
        c.start()
    loads_w[0].start()
    for c in loads_b[1]:
        c.start()
    for c in loads_w[1:]:
        c.start()
    for piece, load in zip(pieces, loads_b[0]):
        load.wait()
        fst[piece] = bv[(0,) + piece].astype(jnp.bfloat16)
    for c in range(CHUNKS):
        v[0, c, j, t, y, k] = fst[t, k, c]

    pl.semaphore_wait(barrier, len(greeted))

    def own_send(m):
        loads_w[m].wait()
        send(w.at[m, t, k], msend.at[m, 0], mrecv.at[m, 0], PAIR)
        send(w.at[m, t, k], msend.at[m, 1], mrecv.at[m, 1], SIB)

    def pass_on(m):
        arrived(w.at[m, u, k], msend.at[m, 0], mrecv.at[m, 0], PAIR)
        send(w.at[m, u, k], msend.at[m, 2], mrecv.at[m, 2], SIB)

    def own_complete(m):
        arrived(w.at[m, t, n], msend.at[m, 1], mrecv.at[m, 1], SIB)

    def pair_complete(m):
        arrived(w.at[m, u, n], msend.at[m, 2], mrecv.at[m, 2], SIB)

    def complete(m):
        own_complete(m)
        pair_complete(m)

    def rows_of(chip, m, s, c):
        total = None
        for jj in range(2):
            for h in range(2):
                first = (h if jj == 0 else 3 - h) * 8 * rows
                lhs = w[m, chip, :, :, first:first + 8 * rows]
                rhs = v[s, c, jj, h].reshape(8 * rows, width)
                part = jnp.dot(lhs.reshape(-1, 8 * rows), rhs, preferred_element_type=jnp.float32)
                total = part if total is None else total + part
        return total

    def product(m, s, c):
        return rows_of(slice(None), m, s, c)

    def near(s, c, e, h):
        ss, rr = vsend.at[s, c], vrecv.at[s, c]
        send(v.at[s, c, j, h, y], ss.at[2, e], rr.at[2, e], UP)
        send(v.at[s, c, j, h, y], ss.at[3, e], rr.at[3, e], DOWN)

    def spread(s, c, halves):
        ss, rr = vsend.at[s, c], vrecv.at[s, c]
        for e, h in halves:
            send(v.at[s, c, j, h, y], ss.at[0, e], rr.at[0, e], FAR)
            send(v.at[s, c, j, h, y], ss.at[1, e], rr.at[1, e], SIDE)
        if halves[0][0] == 0:
            near(s, c, *halves[0])

    def relay(s, c, halves):
        ss, rr = vsend.at[s, c], vrecv.at[s, c]
        for e, h in halves:
            side = v.at[s, c, i, h, y]
            arrived(side, ss.at[1, e], rr.at[1, e], SIDE)
            if e == 0:
                near(s, c, *halves[1])
            send(side, ss.at[5, e], rr.at[5, e], UP)
            send(side, ss.at[6, e], rr.at[6, e], DOWN)
        for e, h in halves:
            far = v.at[s, c, j, h, yo]
            arrived(far, ss.at[0, e], rr.at[0, e], FAR)
            send(far, ss.at[4, e], rr.at[4, e], SIDE)

    def gathered(s, c, halves):
        ss, rr = vsend.at[s, c], vrecv.at[s, c]
        for e, h in halves:
            arrived(v.at[s, c, j, h, yl], ss.at[2, e], rr.at[2, e], DOWN)
            arrived(v.at[s, c, i, h, yl], ss.at[5, e], rr.at[5, e], DOWN)
            arrived(v.at[s, c, j, h, yr], ss.at[3, e], rr.at[3, e], UP)
            arrived(v.at[s, c, i, h, yr], ss.at[6, e], rr.at[6, e], UP)
            arrived(v.at[s, c, i, h, yo], ss.at[4, e], rr.at[4, e], SIDE)

    def residual(s, c, values):
        v[s, c, j, :, y] = values.astype(jnp.bfloat16).reshape(2, 2, rows, width)
        spread(s, c, plain)

    def result_own(s, c, total):
        ob[s, c, t] = total.astype(jnp.bfloat16).reshape(2, rows, width)
        send(ob.at[s, c, t, n], xsend.at[s, c, 2], xrecv.at[s, c, 2], SIB, ro.at[s, c, t, k])
        ro[s, c, t, k] = ob[s, c, t, k]

    def result_pair(s, c, total):
        ob[s, c, u] = total.astype(jnp.bfloat16).reshape(2, rows, width)
        send(ob.at[s, c, u, k], xsend.at[s, c, 0], xrecv.at[s, c, 0], PAIR, ro.at[s, c, t, k])
        send(ob.at[s, c, u, n], xsend.at[s, c, 1], xrecv.at[s, c, 1], CROSS, ro.at[s, c, t, k])

    def write(s, c):
        ss, rr = xsend.at[s, c], xrecv.at[s, c]
        arrived(ro.at[s, c, t, n], ss.at[2], rr.at[2], SIB)
        arrived(ro.at[s, c, u, k], ss.at[0], rr.at[0], PAIR)
        arrived(ro.at[s, c, u, n], ss.at[1], rr.at[1], CROSS)
        for half in range(2):
            for core in range(2):
                first = (half * 2 + core) * cols + c * width
                o[s, :, first:first + width] = ro[s, c, half, core].astype(jnp.float32)

    every = range(CHUNKS)

    def relays(s, halves):
        for c in every:
            relay(s, c, halves)

    for c in every:
        send(fst.at[u, k, c], asend.at[c, 0], arecv.at[c, 0], PAIR, v.at[0, c, j, t, y, k])
        send(fst.at[u, n, c], asend.at[c, 1], arecv.at[c, 1], CROSS, v.at[0, c, j, t, y, k])
        send(fst.at[t, n, c], asend.at[c, 2], arecv.at[c, 2], SIB, v.at[0, c, j, t, y, k])
    own_send(L10)
    for c in loads_b[1]:
        c.wait()
    for c in every:
        send(bv.at[1, u, k, c], bsend.at[c, 0], brecv.at[c, 0], PAIR, b1g.at[c, t, k])
        send(bv.at[1, u, n, c], bsend.at[c, 1], brecv.at[c, 1], CROSS, b1g.at[c, t, k])
        send(bv.at[1, t, n, c], bsend.at[c, 2], brecv.at[c, 2], SIB, b1g.at[c, t, k])
    for m in range(1, 6):
        own_send(m)
    for c in every:
        b1g[c, t, k] = bv[1, t, k, c]
    plain, mine_first = ((0, 0), (1, 1)), ((0, t), (1, u))
    for c in every:
        arrived(v.at[0, c, j, t, y, n], asend.at[c, 2], arecv.at[c, 2], SIB)
        spread(0, c, mine_first[:1])
    for c in every:
        arrived(v.at[0, c, j, u, y, k], asend.at[c, 0], arecv.at[c, 0], PAIR)
        arrived(v.at[0, c, j, u, y, n], asend.at[c, 1], arecv.at[c, 1], CROSS)
        spread(0, c, mine_first[1:])
    relays(0, mine_first)
    pass_on(L10)
    complete(L10)
    for c in every:
        gathered(0, c, mine_first)
        arrived(b1g.at[c, t, n], bsend.at[c, 2], brecv.at[c, 2], SIB)
        arrived(b1g.at[c, u, k], bsend.at[c, 0], brecv.at[c, 0], PAIR)
        arrived(b1g.at[c, u, n], bsend.at[c, 1], brecv.at[c, 1], CROSS)
        start = b1g[c].reshape(own, width)
        residual(1, c, start - product(L10, 0, c))
    relays(1, plain)
    pass_on(LI1)
    complete(LI1)
    for c in every:
        gathered(1, c, plain)
        residual(2, c, product(LI1, 1, c))
    pass_on(LI0)
    relays(2, plain)
    complete(LI0)
    pass_on(U01)
    for c in every:
        y0[c] = product(LI0, 0, c)
    complete(U01)
    for c in every:
        gathered(2, c, plain)
        residual(3, c, y0[c] - product(U01, 2, c))
    pass_on(UI1)
    relays(3, plain)
    own_complete(UI1)
    for c in every:
        result_own(1, c, rows_of(t, UI1, 2, c))
    pair_complete(UI1)
    for c in every:
        result_pair(1, c, rows_of(u, UI1, 2, c))
    own_complete(UI0)
    gathered(3, 0, plain)
    result_own(0, 0, rows_of(t, UI0, 3, 0))
    pass_on(UI0)
    gathered(3, 1, plain)
    result_own(0, 1, rows_of(t, UI0, 3, 1))
    pair_complete(UI0)
    for c in every:
        result_pair(0, c, rows_of(u, UI0, 3, c))
    for s in (1, 0):
        for c in every:
            write(s, c)
    for c in sent:
        c.wait_send()


def shards(lower_coupling, upper_coupling, lower_inverse, upper_inverse, right_side):
    rows = right_side.shape[1]
    cols = right_side.shape[2] // 4
    width = cols // CHUNKS
    f32, bf16 = jnp.float32, jnp.bfloat16
    dma = pltpu.SemaphoreType.DMA
    hbm = pl.BlockSpec(memory_space=pltpu.MemorySpace.HBM)
    return pl.pallas_call(
        kernel,
        out_shape=jax.ShapeDtypeStruct(right_side.shape, f32),
        in_specs=[hbm] * 5,
        out_specs=pl.BlockSpec(memory_space=pltpu.MemorySpace.VMEM),
        scratch_shapes=[
            pltpu.VMEM((6, 2, 2, rows, 32 * rows), bf16),
            pltpu.VMEM((4, CHUNKS, 2, 2, 4, 2, rows, width), bf16),
            pltpu.VMEM((2, 2, 2, CHUNKS, rows, width), f32),
            pltpu.VMEM((2, 2, CHUNKS, rows, width), bf16),
            pltpu.VMEM((CHUNKS, 2, 2, rows, width), f32),
            pltpu.VMEM((CHUNKS, 4 * rows, width), f32),
            pltpu.VMEM((2, CHUNKS, 2, 2, rows, width), bf16),
            pltpu.VMEM((2, CHUNKS, 2, 2, rows, width), bf16),
            dma((3, 8)),
            dma((4, CHUNKS, 7, 2)), dma((4, CHUNKS, 7, 2)),
            dma((6, 3)), dma((6, 3)),
            dma((CHUNKS, 3)), dma((CHUNKS, 3)),
            dma((CHUNKS, 3)), dma((CHUNKS, 3)),
            dma((2, CHUNKS, 3)), dma((2, CHUNKS, 3)),
        ],
        compiler_params=pltpu.CompilerParams(
            collective_id=0, has_side_effects=True, vmem_limit_bytes=53 * 2**20
        ),
    )(lower_coupling, lower_inverse, upper_coupling, upper_inverse, right_side)


def solution(mesh):
    finer = Mesh(mesh.devices.reshape(4, 4, 2, mesh.shape["rhs"]), BLK + ("rhs",))
    spec = P(None, BLK, None)
    return jax.shard_map(
        shards,
        mesh=finer,
        in_specs=(spec, spec, spec, spec, P(None, BLK, "rhs")),
        out_specs=P(None, BLK, "rhs"),
        check_vma=False,
    )
```
